256 devices in a mesh: groups: 4 (over y, x), az: 64 (over z, core).
Axes of the slice: x: 2, y: 2, z: 32, core: 2. Of those that a mesh axis runs over, the one named last changes fastest.
The devices are a block of a 4x8x32 slice.
Arguments:
- sweep_stack: bfloat16 [2, 4, 256, 80, 2560], P(None, None, ('groups', 'az')), parts along dimension 2
- blend_curve: bfloat16 [256, 80], P(('groups', 'az')), parts along dimension 0, may hold values from 0.25 to 4
- sweep_start_index: int32 [256], P(('groups', 'az')), parts along dimension 0, may hold values from -20 to 2530, as said below
- usable_azimuth_extent: int32 [256, 2], P(('groups', 'az')), parts along dimension 0, may hold values from 0 to 80, as said below
- usable_column_extent: int32 [256, 2], P(('groups', 'az')), parts along dimension 0, may hold values from 0 to 2560, as said below
- image_couples: int32 [16, 2], P('groups'), parts along dimension 0, may hold values from 0 to 3, as said below
Outputs:
- interferogram: float32 [2, 16, 512, 128], P(None, 'groups', 'az'), parts along dimension 1
- coherence: float32 [16, 512, 128], P('groups', 'az'), parts along dimension 0
The draws below stay inside these ranges and needn't reach their ends.
There are 4 independent parts, one for each index of `groups`. The reference program is written for one: setup_inputs(seed, part) draws one part's arguments, and reference() takes and returns one part's arrays. A program takes and returns all parts, laid end to end along the dimension named above; each array names one. Nothing has to cross between parts.
Inputs may be any that keep to these rules, and one draw needn't show every extreme that they name: `sweep_start_index`: the valid lines of burst b lie at merged rows from b * 40 - 15 to (b + 1) * 40 + 14, and some burst reaches both ends. The valid lines of all bursts together cover every merged row from 0 to 2559. `usable_azimuth_extent`: first below end for every burst. `usable_column_extent`: first below end for every burst. `image_couples`: the two acquisitions of a pair differ.
All inputs are finite; a program needn't handle non-finite values.
Results may differ from the reference program's by a relative error of at most 0.0003.
Values may be sent and summed in bfloat16 or wider, within the bound.
A program may use at most 64 MiB of HBM per device.

```python
import math
import jax
import jax.numpy as jnp
from jax import lax

BLOCK_HEIGHT = 40
SLANT_WIDTH = 2560
IMAGE_TOTAL = 4
PAIRS = 4
LOOK_ROWS = 5
LOOK_COLS = 20
SHIFT_BOUND_MAX = 10
SPILL_REACH = 5
SWEEP_HEIGHT = 80
SWEEP_TOTAL = 64
GRID_HEIGHT = 2560


def geometry(key):
    seed_stream = jax.random.split(jax.random.fold_in(key, 7), 5)
    index_grid = jnp.arange(SWEEP_TOTAL + 1, dtype=jnp.int32)
    sweep_identifiers = jnp.arange(SWEEP_TOTAL, dtype=jnp.int32)
    edge_shifts = jax.random.randint(seed_stream[0], (SWEEP_TOTAL + 1,), 0 - SHIFT_BOUND_MAX, SHIFT_BOUND_MAX + 1, dtype=jnp.int32)
    peak_amount = jax.random.randint(seed_stream[1], (), 1, SWEEP_TOTAL - 1, dtype=jnp.int32)
    edge_shifts = jnp.where(index_grid == peak_amount, 0 - SHIFT_BOUND_MAX, edge_shifts)
    edge_shifts = jnp.where(index_grid == peak_amount + 1, SHIFT_BOUND_MAX, edge_shifts)
    edge_shifts = jnp.where((index_grid == 0) | (index_grid == SWEEP_TOTAL), 0, edge_shifts)
    sweep_edges = index_grid * BLOCK_HEIGHT + edge_shifts
    south_spill = jax.random.randint(seed_stream[2], (SWEEP_TOTAL,), 1, SPILL_REACH + 1, dtype=jnp.int32)
    south_spill = jnp.where(sweep_identifiers == peak_amount, SPILL_REACH, south_spill)
    north_spill = jax.random.randint(seed_stream[3], (SWEEP_TOTAL,), 1, SPILL_REACH + 1, dtype=jnp.int32)
    north_spill = jnp.where(sweep_identifiers == peak_amount, SPILL_REACH, north_spill)
    head_indices = jax.random.randint(seed_stream[4], (SWEEP_TOTAL,), 0, SPILL_REACH + 1, dtype=jnp.int32)
    start_indices = sweep_edges[:SWEEP_TOTAL] - south_spill - head_indices
    closing_indices = head_indices + south_spill + (sweep_edges[1:] - sweep_edges[:SWEEP_TOTAL]) + north_spill
    return (start_indices, head_indices, closing_indices)


def draw_sweep_start_index(key, part):
    return geometry(key)[0].astype(jnp.int32)


def draw_usable_azimuth_extent(key, part):
    start_indices, head_indices, closing_indices = geometry(key)
    return jnp.stack([head_indices, closing_indices], axis=1).astype(jnp.int32)


def draw_usable_column_extent(key, part):
    seed_stream = jax.random.split(jax.random.fold_in(key, 13), 2)
    least_index = jax.random.randint(seed_stream[0], (SWEEP_TOTAL,), 0, SLANT_WIDTH // 4, dtype=jnp.int32)
    cutoff_index = jax.random.randint(seed_stream[1], (SWEEP_TOTAL,), 0, SLANT_WIDTH // 4, dtype=jnp.int32)
    return jnp.stack([least_index, SLANT_WIDTH - cutoff_index], axis=1).astype(jnp.int32)


def draw_image_couples(key, part):
    seed_stream = jax.random.split(jax.random.fold_in(key, 17), 2)
    first_acq = jax.random.randint(seed_stream[0], (PAIRS,), 0, IMAGE_TOTAL, dtype=jnp.int32)
    step_acq = jax.random.randint(seed_stream[1], (PAIRS,), 1, IMAGE_TOTAL, dtype=jnp.int32)
    return jnp.stack([first_acq, (first_acq + step_acq) % IMAGE_TOTAL], axis=1).astype(jnp.int32)


def draw_sweep_stack(key, part):
    seed_stream = jax.random.split(jax.random.fold_in(key, 11), 4)
    result_dims = (2, IMAGE_TOTAL, SWEEP_TOTAL, SWEEP_HEIGHT, SLANT_WIDTH)
    common_indices = jax.random.normal(seed_stream[0], (2, 1, SWEEP_TOTAL, SWEEP_HEIGHT, SLANT_WIDTH), jnp.float32)
    single = jax.random.normal(seed_stream[1], result_dims, jnp.float32)
    mixture = 0.7 * (common_indices + single)
    azimuth_scale = jnp.exp(jax.random.uniform(seed_stream[2], (SWEEP_TOTAL, SWEEP_HEIGHT), jnp.float32, -0.7, 0.7))
    sample_scale = jnp.exp(jax.random.uniform(seed_stream[3], (SLANT_WIDTH,), jnp.float32, -0.7, 0.7))
    scaled = mixture * azimuth_scale[None, None, :, :, None] * sample_scale
    return scaled.astype(jnp.bfloat16)


def steps_of(stream_key, dims, pieces, smallest, top_value):
    factor_of = 1.0
    for position, parts in pieces:
        draws = jax.random.uniform(jax.random.fold_in(jax.random.fold_in(stream_key, 6), position), (parts,), jnp.float32, smallest / len(pieces), top_value / len(pieces))
        factor_of = factor_of * jnp.repeat(jnp.exp(draws), dims[position] // parts).reshape((-1,) + (1,) * (len(dims) - 1 - position))
    return factor_of


def setup_inputs(seed: int = 0, part: int = 0) -> dict:
    keys = jax.random.split(jax.random.key(seed), 7)
    part_splits = jax.random.split(jax.random.fold_in(keys[6], part), 7)
    sweep_stack = draw_sweep_stack(jax.random.fold_in(jax.random.fold_in(keys[6], part), 71), part)
    blend_curve = jnp.clip(jnp.exp(math.log(4.0) - 2.7725887 * jax.random.uniform(part_splits[1], (SWEEP_TOTAL, SWEEP_HEIGHT), jnp.float32) ** steps_of(part_splits[1], (SWEEP_TOTAL, SWEEP_HEIGHT), ((0, 64),), -0.2, 0.2)), 0.25, 4.0).astype(jnp.bfloat16)
    sweep_start_index = draw_sweep_start_index(jax.random.fold_in(jax.random.fold_in(keys[6], part), 71), part)
    usable_azimuth_extent = draw_usable_azimuth_extent(jax.random.fold_in(jax.random.fold_in(keys[6], part), 71), part)
    usable_column_extent = draw_usable_column_extent(jax.random.fold_in(jax.random.fold_in(keys[6], part), 71), part)
    image_couples = draw_image_couples(jax.random.fold_in(jax.random.fold_in(keys[6], part), 71), part)
    return dict(sweep_stack=sweep_stack, blend_curve=blend_curve, sweep_start_index=sweep_start_index, usable_azimuth_extent=usable_azimuth_extent, usable_column_extent=usable_column_extent, image_couples=image_couples)


def box_sums(values):
    shaped = values.reshape(values.shape[:-2] + (GRID_HEIGHT // LOOK_ROWS, LOOK_ROWS, SLANT_WIDTH // LOOK_COLS, LOOK_COLS))
    return jnp.sum(shaped, axis=(-3, -1))


def reference(sweep_stack, blend_curve, sweep_start_index, usable_azimuth_extent, usable_column_extent, image_couples):
    azimuth_index = jnp.arange(SWEEP_HEIGHT, dtype=jnp.int32)
    column_index = jnp.arange(SLANT_WIDTH, dtype=jnp.int32)
    reference_point = jnp.zeros((), jnp.int32)
    cross_term = jnp.zeros((2, IMAGE_TOTAL, GRID_HEIGHT + 2 * SWEEP_HEIGHT, SLANT_WIDTH), jnp.float32)
    intensity_norm = jnp.zeros((GRID_HEIGHT + 2 * SWEEP_HEIGHT,), jnp.float32)

    def deposit_sweep(sweep_index, cumulative_sums):
        aggregate, blend_total = cumulative_sums
        sweep_content = lax.dynamic_index_in_dim(sweep_stack, sweep_index, 2, keepdims=False)
        usable_marks = (azimuth_index >= usable_azimuth_extent[sweep_index, 0]) & (azimuth_index < usable_azimuth_extent[sweep_index, 1])
        azimuth_blend = jnp.where(usable_marks, blend_curve[sweep_index], jnp.zeros((), jnp.bfloat16)).astype(jnp.float32)
        column_usable = ((column_index >= usable_column_extent[sweep_index, 0]) & (column_index < usable_column_extent[sweep_index, 1])).astype(jnp.float32)
        added_term = sweep_content.astype(jnp.float32) * azimuth_blend[:, None] * column_usable[None, :]
        start_index = (sweep_start_index[sweep_index] + SWEEP_HEIGHT).astype(jnp.int32)
        available = lax.dynamic_slice(aggregate, (reference_point, reference_point, start_index, reference_point), (2, IMAGE_TOTAL, SWEEP_HEIGHT, SLANT_WIDTH))
        aggregate = lax.dynamic_update_slice(aggregate, available + added_term, (reference_point, reference_point, start_index, reference_point))
        available_blends = lax.dynamic_slice(blend_total, (start_index,), (SWEEP_HEIGHT,))
        blend_total = lax.dynamic_update_slice(blend_total, available_blends + azimuth_blend, (start_index,))
        return aggregate, blend_total

    cross_term, intensity_norm = lax.fori_loop(0, SWEEP_TOTAL, deposit_sweep, (cross_term, intensity_norm))
    combined_grid = cross_term[:, :, SWEEP_HEIGHT:SWEEP_HEIGHT + GRID_HEIGHT] / intensity_norm[SWEEP_HEIGHT:SWEEP_HEIGHT + GRID_HEIGHT][:, None]
    intensity = combined_grid[0] * combined_grid[0] + combined_grid[1] * combined_grid[1]
    first_image = jnp.take(combined_grid, image_couples[:, 0], axis=1)
    second_image = jnp.take(combined_grid, image_couples[:, 1], axis=1)
    real_part = first_image[0] * second_image[0] + first_image[1] * second_image[1]
    imag_part = first_image[1] * second_image[0] - first_image[0] * second_image[1]
    look_sum = box_sums(jnp.stack([real_part, imag_part]))
    look_power = box_sums(intensity)
    power_first = jnp.take(look_power, image_couples[:, 0], axis=0)
    power_second = jnp.take(look_power, image_couples[:, 1], axis=0)
    coherence = (look_sum[0] * look_sum[0] + look_sum[1] * look_sum[1]) / jnp.maximum(power_first * power_second, 1.0)
    interferogram = look_sum / (LOOK_ROWS * LOOK_COLS)
    return interferogram, coherence
```

```python
import functools

import jax
import jax.numpy as jnp
from jax import lax
from jax.experimental import pallas as pl
from jax.experimental.pallas import tpu as pltpu
from jax.sharding import PartitionSpec as P

BLOCK_HEIGHT = 40
LOOK_ROWS = 5
LOOK_COLS = 20
MARGIN = 15
LANES = 256
CHUNK = 2 * LANES
SUB = 16
F32, BF16, I32 = jnp.float32, jnp.bfloat16, jnp.int32


def iota(shape, dimension):
    return lax.broadcasted_iota(I32, shape, dimension)


def own_row(position):
    looks = BLOCK_HEIGHT // LOOK_ROWS
    return LOOK_ROWS * (position % looks) + position // looks


def kernel(
    ring,
    x_hbm,
    blend_hbm,
    start_hbm,
    lines_hbm,
    columns_hbm,
    couples_hbm,
    ifg_ref,
    coh_ref,
    x,
    stage,
    recv,
    own,
    spread,
    boxes,
    total,
    note,
    heard,
    blend,
    start,
    lines,
    columns,
    couples,
    x_sem,
    small_sem,
    send_sem,
    recv_sem,
    note_send,
    note_recv,
):
    chunks, planes, height, _ = x.shape
    images = planes // 2
    duos = [(i, j) for i in range(images) for j in range(i + 1, images)]
    pairs = couples.shape[1]
    looks = BLOCK_HEIGHT // LOOK_ROWS
    me = lax.axis_index("az")
    above, below = lax.rem(me + ring - 1, ring), lax.rem(me + 1, ring)
    targets = (above, below)

    small = [
        pltpu.make_async_copy(source, target, small_sem.at[i])
        for i, (source, target) in enumerate(
            (
                (blend_hbm, blend),
                (start_hbm, start),
                (lines_hbm, lines),
                (columns_hbm, columns),
                (couples_hbm, couples),
            )
        )
    ]
    for copy in small:
        copy.start()
    loads = [
        pltpu.make_async_copy(
            x_hbm.at[:, :, pl.ds(c * CHUNK, CHUNK)], x.at[c], x_sem.at[c]
        )
        for c in range(chunks)
    ]
    for copy in loads:
        copy.start()

    barrier = pltpu.get_barrier_semaphore()
    for target in targets:
        pl.semaphore_signal(
            barrier, inc=1, device_id={"az": target}, device_id_type=pl.DeviceIdType.MESH
        )

    for copy in small:
        copy.wait()
    shift = start[0, 0] - me * BLOCK_HEIGHT
    line = iota((1, height), 1)
    valid = (line >= lines[0, 0]) & (line < lines[0, 1])
    weight = jnp.where(valid, blend[...].astype(F32), 0.0)

    far = planes - 1
    absent = -1000
    bases = (-MARGIN, BLOCK_HEIGHT)

    def own_target(rows, first):
        return own_row(iota((rows, 1), 0) - first)

    def selection(rows, target, first_own):
        row = iota((rows, 1), 0)
        matches = (iota((rows, height), 1) + shift) == target
        values = jnp.where(row < first_own, 1.0, weight)
        return jnp.where(matches, values, 0.0)

    row = iota((2 * SUB + BLOCK_HEIGHT, 1), 0)
    tile_row = row % SUB
    target = jnp.where(row < SUB, bases[0], bases[1]) + tile_row
    target = jnp.where(tile_row == MARGIN, absent, target)
    target = jnp.where(row >= 2 * SUB, own_target(row.shape[0], 2 * SUB), target)
    select_near_f32 = selection(row.shape[0], target, 2 * SUB)
    select_near = select_near_f32.astype(BF16)
    rest = SUB // 2
    groups = rest * far
    far_own = 2 * rest + 2 * groups
    row = iota((far_own + BLOCK_HEIGHT, 1), 0)
    sub = row % rest
    up_side = (row < rest) | ((row >= 2 * rest) & (row < 2 * rest + groups))
    member = jnp.where(up_side, row - 2 * rest, row - 2 * rest - groups) // rest
    offset = jnp.where(row < 2 * rest, far + sub, jnp.where(sub == rest - 1, member, absent))
    target = jnp.where(up_side, bases[0], bases[1]) + offset
    target = jnp.where(row >= far_own, own_target(row.shape[0], far_own), target)
    select_far = selection(row.shape[0], target, far_own).astype(BF16)

    lane = iota((1, LANES), 1)
    side, place = lane // (LANES // 2), lane % (LANES // 2)
    tile, inner = place // SUB, place % SUB

    def origin(half):
        tail = inner - rest * half
        in_tail = tile == far
        kept = jnp.logical_not(in_tail) | ((tail >= 0) & (tail < rest))
        plane = jnp.where(in_tail | (inner == MARGIN), far, tile)
        offset = jnp.where(in_tail, far + tail, jnp.where(inner == MARGIN, tile, inner))
        return jnp.where(kept, plane, absent), offset

    eight = jnp.broadcast_to(weight, (8, height)).astype(BF16)
    for half in range(2):
        _, offset = origin(half)
        wanted = jnp.where(side == 0, bases[1], bases[0]) + offset
        picks = (iota((height, LANES), 0) + shift) == wanted
        sent = jnp.dot(
            eight, jnp.where(picks, 1.0, 0.0).astype(BF16), preferred_element_type=F32
        )
        note[1, pl.ds(8 * half, 8), :] = sent[:, : LANES // 2]
        note[0, pl.ds(8 * half, 8), :] = sent[:, LANES // 2 :]

    pl.semaphore_wait(barrier, 2)
    notes = [
        pltpu.make_async_remote_copy(
            src_ref=note.at[d],
            dst_ref=heard.at[1 - d],
            send_sem=note_send.at[d],
            recv_sem=note_recv.at[1 - d],
            device_id={"az": targets[d]},
            device_id_type=pl.DeviceIdType.MESH,
        )
        for d in range(2)
    ]

    def message(d, c):
        return pltpu.make_async_remote_copy(
            src_ref=stage.at[d, c],
            dst_ref=recv.at[1 - d, c],
            send_sem=send_sem.at[d, c],
            recv_sem=recv_sem.at[1 - d, c],
            device_id={"az": targets[d]},
            device_id_type=pl.DeviceIdType.MESH,
        )

    for copy in notes:
        copy.start()

    def outgoing(c, carry):
        pltpu.make_async_copy(
            x_hbm.at[:, :, pl.ds(pl.multiple_of(c * CHUNK, CHUNK), CHUNK)], x.at[c], x_sem.at[c]
        ).wait()
        column = iota((1, CHUNK), 1) + c * CHUNK
        seen = (column >= columns[0, 0]) & (column < columns[0, 1])
        mask = jnp.where(seen, 1.0, 0.0).astype(BF16)

        def product(matrix, p):
            return jnp.dot(matrix, x[c, p] * mask, preferred_element_type=F32)

        last = product(select_far, far)
        own[c, far] = last[far_own:]
        for d in range(2):
            tail = last[d * rest : (d + 1) * rest]
            stage[d, c, 2 * far] = jnp.concatenate(
                [tail[:, :LANES], tail[:, LANES:]], axis=0
            ).astype(BF16)
        for p in range(far):
            near = product(select_near, p)
            own[c, p] = near[2 * SUB :]
            for d in range(2):
                extra = 2 * rest + d * groups + rest * p
                block = jnp.concatenate(
                    [
                        near[d * SUB : d * SUB + rest],
                        near[d * SUB + rest : (d + 1) * SUB] + last[extra : extra + rest],
                    ],
                    axis=0,
                ).astype(BF16)
                stage[d, c, p] = block[:, :LANES]
                stage[d, c, far + p] = block[:, LANES:]
        for d in range(2):
            message(d, c).start()
        return carry

    lax.fori_loop(0, chunks, outgoing, 0)

    def box(c, carry):
        sample = iota((LANES, 128), 0) + c * LANES
        first = LOOK_COLS * iota((LANES, 128), 1)
        inside = (sample >= first) & (sample < first + LOOK_COLS)
        boxes[c] = jnp.where(inside, 1.0, 0.0).astype(BF16)
        return carry

    lax.fori_loop(0, 2 * chunks, box, 0)
    total[...] = jnp.zeros_like(total)

    for copy in notes:
        copy.wait()
    has = (
        jnp.where(me > 0, 1.0, 0.0).astype(F32),
        jnp.where(me < ring - 1, 1.0, 0.0).astype(F32),
    )
    norm = jnp.sum(select_near_f32[2 * SUB :], axis=1, keepdims=True)
    row_code = own_row(iota((BLOCK_HEIGHT, 1), 0))
    for half in range(2):
        plane, offset = origin(half)
        code = offset + jnp.where(side == 0, 0, BLOCK_HEIGHT - MARGIN)
        weights = jnp.concatenate(
            [heard[d, 8 * half : 8 * half + 1, :] * has[d] for d in range(2)], axis=1
        )
        for p in range(planes):
            matches = (row_code == code) & (plane == p)
            block = jnp.where(matches, weights, 0.0)
            spread[half, pl.ds(p * BLOCK_HEIGHT, BLOCK_HEIGHT), :] = block.astype(BF16)
            if half == 0 and p == 0:
                norm = norm + jnp.sum(block, axis=1, keepdims=True)
    scale = jnp.broadcast_to(1.0 / norm, (BLOCK_HEIGHT, LANES))

    def incoming(c, carry):
        for d in range(2):
            message(d, c).wait_recv()
        for half in range(2):
            tiles = []
            for d in range(2):
                tiles.append(recv[d, c, pl.ds(far * half, far)].reshape(far * SUB, LANES))
                tiles.append(recv[d, c, 2 * far])
            spill = jnp.dot(
                spread[half], jnp.concatenate(tiles, axis=0), preferred_element_type=F32
            )
            sums = [None] * (2 * len(duos) + images)

            def gather(slot, value):
                sums[slot] = value if sums[slot] is None else sums[slot] + value

            for within in range(LOOK_ROWS):
                rows = pl.ds(within * looks, looks)
                merged = []
                for p in range(planes):
                    at = p * BLOCK_HEIGHT + within * looks
                    merged.append(
                        (spill[at : at + looks] + own[c, p, rows, pl.ds(half * LANES, LANES)])
                        * scale[within * looks : (within + 1) * looks]
                    )
                re, im = merged[:images], merged[images:]
                for slot, (i, j) in enumerate(duos):
                    gather(slot, re[i] * re[j] + im[i] * im[j])
                    gather(len(duos) + slot, im[i] * re[j] - re[i] * im[j])
                for i in range(images):
                    gather(2 * len(duos) + i, re[i] * re[i] + im[i] * im[i])
            sums = jnp.concatenate(sums, axis=0)
            high = sums.astype(BF16)
            low = (sums - high.astype(F32)).astype(BF16)
            box_matrix = boxes[2 * c + half]
            total[...] += jnp.dot(high, box_matrix, preferred_element_type=F32) + jnp.dot(
                low, box_matrix, preferred_element_type=F32
            )
        return carry

    lax.fori_loop(0, chunks, incoming, 0)

    def looked(slot):
        return total[pl.ds(slot * looks, looks), :]

    def splat(value):
        return jnp.full((looks, total.shape[1]), value, I32)

    for p in range(pairs):
        i, j = splat(couples[0, p]), splat(couples[1, p])
        re = im = jnp.zeros(i.shape, F32)
        power_i = power_j = jnp.zeros(i.shape, F32)
        for slot, (a, b) in enumerate(duos):
            forward = (i == a) & (j == b)
            backward = (i == b) & (j == a)
            re = jnp.where(forward | backward, looked(slot), re)
            im = jnp.where(forward, looked(len(duos) + slot), im)
            im = jnp.where(backward, -looked(len(duos) + slot), im)
        for a in range(images):
            power_i = jnp.where(i == a, looked(2 * len(duos) + a), power_i)
            power_j = jnp.where(j == a, looked(2 * len(duos) + a), power_j)
        ifg_ref[0, p] = re / (LOOK_ROWS * LOOK_COLS)
        ifg_ref[1, p] = im / (LOOK_ROWS * LOOK_COLS)
        coh_ref[p] = (re * re + im * im) / jnp.maximum(power_i * power_j, 1.0)

    def drain(c, carry):
        for d in range(2):
            message(d, c).wait_send()
        return carry

    lax.fori_loop(0, chunks, drain, 0)


def per_device(ring, sweep_stack, blend, start, lines, columns, couples):
    parts, images, _, height, width = sweep_stack.shape
    planes = parts * images
    pairs = couples.shape[0]
    chunks = width // CHUNK
    looks = BLOCK_HEIGHT // LOOK_ROWS
    outputs = width // LOOK_COLS
    tiles = 2 * planes - 1
    hbm = pl.BlockSpec(memory_space=pltpu.HBM)
    vmem = pl.BlockSpec(memory_space=pltpu.VMEM)
    return pl.pallas_call(
        functools.partial(kernel, ring),
        name="merge",
        out_shape=(
            jax.ShapeDtypeStruct((parts, pairs, looks, outputs), F32),
            jax.ShapeDtypeStruct((pairs, looks, outputs), F32),
        ),
        in_specs=[hbm] * 6,
        out_specs=(vmem, vmem),
        scratch_shapes=[
            pltpu.VMEM((chunks, planes, height, CHUNK), BF16),
            pltpu.VMEM((2, chunks, tiles, SUB, LANES), BF16),
            pltpu.VMEM((2, chunks, tiles, SUB, LANES), BF16),
            pltpu.VMEM((chunks, planes, BLOCK_HEIGHT, CHUNK), F32),
            pltpu.VMEM((2, planes * BLOCK_HEIGHT, LANES), BF16),
            pltpu.VMEM((2 * chunks, LANES, outputs), BF16),
            pltpu.VMEM((images * images * looks, outputs), F32),
            pltpu.VMEM((2, 16, 128), F32),
            pltpu.VMEM((2, 16, 128), F32),
            pltpu.VMEM((1, height), BF16),
            pltpu.SMEM((1, 1), I32),
            pltpu.SMEM((1, 2), I32),
            pltpu.SMEM((1, 2), I32),
            pltpu.SMEM((2, pairs), I32),
            pltpu.SemaphoreType.DMA((chunks,)),
            pltpu.SemaphoreType.DMA((5,)),
            pltpu.SemaphoreType.DMA((2, chunks)),
            pltpu.SemaphoreType.DMA((2, chunks)),
            pltpu.SemaphoreType.DMA((2,)),
            pltpu.SemaphoreType.DMA((2,)),
        ],
        compiler_params=pltpu.CompilerParams(
            collective_id=0, has_side_effects=True
        ),
    )(
        sweep_stack.reshape(planes, height, width),
        blend,
        start.reshape(1, 1),
        lines,
        columns,
        couples.T,
    )


def solution(mesh):
    return jax.shard_map(
        functools.partial(per_device, mesh.shape["az"]),
        mesh=mesh,
        in_specs=(
            P(None, None, ("groups", "az"), None, None),
            P(("groups", "az"), None),
            P(("groups", "az")),
            P(("groups", "az"), None),
            P(("groups", "az"), None),
            P("groups", None),
        ),
        out_specs=(P(None, "groups", "az", None), P("groups", "az", None)),
        check_vma=False,
    )
```

```python
import functools

import jax
import jax.numpy as jnp
from jax import lax
from jax.experimental import pallas as pl
from jax.experimental.pallas import tpu as pltpu
from jax.sharding import PartitionSpec as P

BLOCK_HEIGHT = 40
LOOK_ROWS = 5
LOOK_COLS = 20
MARGIN = 15
HALF = 256
CHUNK = 2 * HALF
SUB = 16
SIDES = 2
F32, BF16, I32 = jnp.float32, jnp.bfloat16, jnp.int32
MESH = pl.DeviceIdType.MESH


def iota(shape, dimension):
    return lax.broadcasted_iota(I32, shape, dimension)


def dot(a, b):
    return jnp.dot(a, b, preferred_element_type=F32)


def swap(block):
    half = block.shape[0] // 2
    return jnp.concatenate([block[half:], block[:half]], axis=0)


def merge(
    ring,
    x_hbm,
    blend_hbm,
    start_hbm,
    lines_hbm,
    columns_hbm,
    couples_hbm,
    ifg_ref,
    coh_ref,
    x,
    stage,
    recv,
    own,
    spread,
    boxes,
    spilled,
    split,
    total,
    note,
    heard,
    blend,
    start,
    lines,
    columns,
    couples,
    x_sem,
    small_sem,
    send_sem,
    recv_sem,
    note_send,
    note_recv,
    hello,
):
    chunks, planes, height, _ = x.shape
    images = planes // 2
    pairs = couples.shape[1]
    looks = BLOCK_HEIGHT // LOOK_ROWS
    quads = looks // SIDES
    duos = [(i, j) for i in range(images) for j in range(i + 1, images)]
    me = lax.axis_index("az")
    above, below = lax.rem(me + ring - 1, ring), lax.rem(me + 1, ring)
    targets = (above, below)
    present = (me > 0, me < ring - 1)

    small = [
        pltpu.make_async_copy(source, target, small_sem.at[i])
        for i, (source, target) in enumerate(
            (
                (start_hbm, start),
                (columns_hbm, columns),
                (lines_hbm, lines),
                (blend_hbm, blend),
                (couples_hbm, couples),
            )
        )
    ]

    def load(c):
        return pltpu.make_async_copy(
            x_hbm.at[:, :, pl.ds(c * CHUNK, CHUNK)], x.at[c], x_sem.at[c]
        )

    for copy in small[:3]:
        copy.start()
    load(0).start()
    for copy in small[3:]:
        copy.start()
    for c in range(1, chunks):
        load(c).start()

    barrier = pltpu.get_barrier_semaphore()

    @pl.when(present[0])
    def _():
        pl.semaphore_signal(barrier, inc=1, device_id={"az": above}, device_id_type=MESH)

    for side in range(SIDES):

        @pl.when(jnp.logical_not(present[side]))
        def _():
            heard[side] = jnp.zeros(heard.shape[1:], F32)
            for c in range(chunks):
                recv[side, c] = jnp.zeros(recv.shape[2:], BF16)

    def outgoing(side, c):
        return pltpu.make_async_remote_copy(
            src_ref=stage.at[side, c],
            dst_ref=recv.at[1 - side, c],
            send_sem=send_sem.at[side, c],
            recv_sem=recv_sem.at[1 - side, c],
            device_id={"az": targets[side]},
            device_id_type=MESH,
        )

    def words(side):
        return pltpu.make_async_remote_copy(
            src_ref=note.at[side],
            dst_ref=heard.at[1 - side],
            send_sem=note_send.at[side],
            recv_sem=note_recv.at[1 - side],
            device_id={"az": targets[side]},
            device_id_type=MESH,
        )

    for copy in small[:2]:
        copy.wait()
    shift = start[0, 0] - me * BLOCK_HEIGHT
    bases = (-MARGIN, BLOCK_HEIGHT)

    place = iota((1, 2 * height), 1)
    second = place >= height
    line = jnp.where(second, place - height, place)
    row_of_line = line + shift

    lead = iota((SIDES * 2 * SUB, 1), 0)
    inner = lead % SUB
    leaves = jnp.where(lead < 2 * SUB, bases[0], bases[1]) + inner
    wanted = row_of_line == jnp.where(inner < MARGIN, leaves, -1000)
    half_matches = second == (lead % (2 * SUB) >= SUB)
    select = jnp.where(wanted & half_matches, 1.0, 0.0).astype(BF16)

    def masks(c):
        column = iota((1, CHUNK), 1) + c * CHUNK
        seen = (column >= columns[0, 0]) & (column < columns[0, 1])
        return jnp.where(seen, 1.0, 0.0).astype(BF16)

    def stacked(block):
        return jnp.concatenate([block[:, :HALF], block[:, HALF:]], axis=0)

    def prepare(c):
        load(c).wait()
        mask = masks(c)
        for p in range(planes):
            block = x[c, p] * mask
            x[c, p] = block
            out = dot(select, stacked(block)).astype(BF16)
            for side in range(SIDES):
                stage[side, c, pl.ds(2 * p * SUB, 2 * SUB), :] = out[
                    side * 2 * SUB : (side + 1) * 2 * SUB
                ]

    prepare(0)

    for copy in small[2:]:
        copy.wait()
    index = iota((1, height), 1)
    valid = (index >= lines[0, 0]) & (index < lines[0, 1])
    weight = jnp.where(valid, blend[...].astype(F32), 0.0)

    k = iota((height, 2 * HALF), 0)
    lane = iota((height, 2 * HALF), 1)
    inner = lane % SUB
    leaves = jnp.where(lane < HALF + HALF // 2, bases[0], bases[1]) + inner
    goes = (lane >= HALF) & (inner < MARGIN) & (k + shift == leaves)
    stays = (lane < HALF) & ((lane == k) | (lane == k + height))
    rows = jnp.broadcast_to(weight, (8, height)).astype(BF16)
    weights = dot(rows, jnp.where(goes | stays, 1.0, 0.0).astype(BF16))
    for side in range(SIDES):
        first = HALF + side * (HALF // 2)
        note[side] = weights[:, first : first + HALF // 2]
    twice = weights[:1, : 2 * height]

    @pl.when(present[1])
    def _():
        pl.semaphore_wait(barrier, 1)
        pl.semaphore_signal(hello, inc=1, device_id={"az": below}, device_id_type=MESH)
        words(1).start()
        outgoing(1, 0).start()

    for c in range(1, chunks):
        prepare(c)

        @pl.when(present[1])
        def _():
            outgoing(1, c).start()

    slot = iota((BLOCK_HEIGHT, 1), 0)
    quad = slot % quads
    second_slot = slot % looks >= quads
    row_in_side = LOOK_ROWS * quad + slot // looks
    keep_f32 = [
        jnp.where(
            (row_of_line == row_in_side + side * quads * LOOK_ROWS) & (second == second_slot),
            twice,
            0.0,
        )
        for side in range(SIDES)
    ]
    keep = jnp.concatenate(keep_f32, axis=0).astype(BF16)

    @pl.when(present[0])
    def _():
        pl.semaphore_wait(hello, 1)
        words(0).start()
        for c in range(chunks):
            outgoing(0, c).start()

    def held(c, carry):
        for p in range(planes):
            out = dot(keep, stacked(x[c, p]))
            for side in range(SIDES):
                own[side, c, p] = out[side * BLOCK_HEIGHT : (side + 1) * BLOCK_HEIGHT]
        return carry

    lax.fori_loop(0, chunks, held, 0)

    def box(c, carry):
        lane = iota((HALF, HALF), 1)
        far = lane >= HALF // 2
        sample = iota((HALF, HALF), 0) + c * CHUNK + jnp.where(far, HALF, 0)
        first = LOOK_COLS * jnp.where(far, lane - HALF // 2, lane)
        inside = (sample >= first) & (sample < first + LOOK_COLS)
        boxes[c] = jnp.where(inside, 1.0, 0.0).astype(BF16)
        return carry

    lax.fori_loop(0, chunks, box, 0)

    def settle(s, carry):
        side = lax.rem(me + s, 2)
        there = (side == 0) & present[0] | (side == 1) & present[1]

        @pl.when(there)
        def _():
            pltpu.make_async_remote_copy(
                src_ref=note.at[side],
                dst_ref=heard.at[side],
                send_sem=note_send.at[side],
                recv_sem=note_recv.at[side],
                device_id={"az": below},
                device_id_type=MESH,
            ).wait_recv()

        lane = iota((1, HALF), 1)
        tile, inner = lane // SUB, lane % SUB
        code = (tile % 2) * 64 + inner + side * LOOK_ROWS
        row_code = jnp.where(second_slot, 64, 0) + row_in_side
        matches = row_code == code
        incoming = jnp.concatenate([heard[side, :1, :]] * 2, axis=1)
        block = jnp.where(matches, incoming, 0.0)
        norm = jnp.sum(jnp.where(tile < 2, block, 0.0), axis=1, keepdims=True)
        stay = jnp.where(side == 0, keep_f32[0], keep_f32[1])
        norm = norm + jnp.sum(stay, axis=1, keepdims=True)
        scale = jnp.broadcast_to(1.0 / norm, (BLOCK_HEIGHT, HALF // 2))
        for p in range(planes):
            spread[pl.ds(p * BLOCK_HEIGHT, BLOCK_HEIGHT), :] = jnp.where(
                tile // 2 == p, block, 0.0
            ).astype(BF16)

        def arrive(c):
            @pl.when(there)
            def _():
                pltpu.make_async_remote_copy(
                    src_ref=stage.at[side, c],
                    dst_ref=recv.at[side, c],
                    send_sem=send_sem.at[side, c],
                    recv_sem=recv_sem.at[side, c],
                    device_id={"az": below},
                    device_id_type=MESH,
                ).wait_recv()

        def spill(c):
            spilled[c % 2] = dot(spread[...], recv[side, c])

        def products(c):
            for b in range(2):
                lanes = pl.ds(b * (HALF // 2), HALF // 2)
                sums = [None] * (images * images)

                def gather(at, value):
                    sums[at] = value if sums[at] is None else sums[at] + value

                for within in range(LOOK_ROWS):
                    own_rows = pl.ds(within * looks, looks)
                    factor = scale[within * looks : (within + 1) * looks]
                    merged = [
                        (
                            spilled[c % 2, pl.ds(p * BLOCK_HEIGHT + within * looks, looks), lanes]
                            + own[side, c, p, own_rows, lanes]
                        )
                        * factor
                        for p in range(planes)
                    ]
                    re, im = merged[:images], merged[images:]
                    for at, (i, j) in enumerate(duos):
                        gather(at, re[i] * re[j] + im[i] * im[j])
                        gather(len(duos) + at, im[i] * re[j] - re[i] * im[j])
                    for i in range(images):
                        gather(2 * len(duos) + i, re[i] * re[i] + im[i] * im[i])
                for at in range(0, images * images, 2):
                    value = jnp.concatenate(sums[at : at + 2], axis=0)
                    high = value.astype(BF16)
                    low = (value - high.astype(F32)).astype(BF16)
                    split[c % 2, 0, pl.ds(at * looks, 2 * looks), lanes] = high
                    split[c % 2, 1, pl.ds(at * looks, 2 * looks), lanes] = low

        def boxed(c):
            part = dot(split[c % 2, 0], boxes[c]) + dot(split[c % 2, 1], boxes[c])
            total[side] = part if c == 0 else total[side] + part

        for c in range(chunks + 2):
            if c < chunks:
                arrive(c)
                spill(c)
            if 1 <= c <= chunks:
                products(c - 1)
            if c >= 2:
                boxed(c - 2)
        return carry

    lax.fori_loop(0, SIDES, settle, 0)

    first_quads = iota((looks, HALF // 2), 0) < quads

    def looked(at):
        rows = pl.ds(at * looks, looks)
        left = [total[side, rows, pl.ds(0, HALF // 2)] for side in range(SIDES)]
        right = [total[side, rows, pl.ds(HALF // 2, HALF // 2)] for side in range(SIDES)]
        return jnp.where(first_quads, left[0] + swap(right[0]), swap(left[1]) + right[1])

    values = [looked(at) for at in range(images * images)]

    def splat(value):
        return jnp.full((looks, HALF // 2), value, I32)

    for p in range(pairs):
        i, j = splat(couples[0, p]), splat(couples[1, p])
        re = im = power_i = power_j = jnp.zeros(i.shape, F32)
        for at, (a, b) in enumerate(duos):
            forward = (i == a) & (j == b)
            backward = (i == b) & (j == a)
            re = jnp.where(forward | backward, values[at], re)
            im = jnp.where(forward, values[len(duos) + at], im)
            im = jnp.where(backward, -values[len(duos) + at], im)
        for a in range(images):
            power_i = jnp.where(i == a, values[2 * len(duos) + a], power_i)
            power_j = jnp.where(j == a, values[2 * len(duos) + a], power_j)
        ifg_ref[0, p] = re / (LOOK_ROWS * LOOK_COLS)
        ifg_ref[1, p] = im / (LOOK_ROWS * LOOK_COLS)
        coh_ref[p] = (re * re + im * im) / jnp.maximum(power_i * power_j, 1.0)

    for side in range(SIDES):

        @pl.when(present[side])
        def _():
            words(side).wait_send()
            for c in range(chunks):
                outgoing(side, c).wait_send()


def write(ifg_ref, coh_ref, ifg_hbm, coh_hbm, sems):
    copies = [
        pltpu.make_async_copy(ifg_ref, ifg_hbm, sems.at[0]),
        pltpu.make_async_copy(coh_ref, coh_hbm, sems.at[1]),
    ]
    for copy in copies:
        copy.start()
    for copy in copies:
        copy.wait()


def per_device(ring, sweep_stack, blend, start, lines, columns, couples):
    parts, images, _, height, width = sweep_stack.shape
    planes = parts * images
    pairs = couples.shape[0]
    chunks = width // CHUNK
    looks = BLOCK_HEIGHT // LOOK_ROWS
    outputs = width // LOOK_COLS
    hbm = pl.BlockSpec(memory_space=pltpu.HBM)
    vmem = pl.BlockSpec(memory_space=pltpu.VMEM)
    ifg_shape, coh_shape = (parts, pairs, looks, outputs), (pairs, looks, outputs)
    ifg, coh = pl.pallas_call(
        functools.partial(merge, ring),
        name="merge",
        out_shape=(pltpu.VMEM(ifg_shape, F32), pltpu.VMEM(coh_shape, F32)),
        in_specs=[hbm] * 6,
        out_specs=(vmem, vmem),
        scratch_shapes=[
            pltpu.VMEM((chunks, planes, height, CHUNK), BF16),
            pltpu.VMEM((SIDES, chunks, planes * 2 * SUB, HALF), BF16),
            pltpu.VMEM((SIDES, chunks, planes * 2 * SUB, HALF), BF16),
            pltpu.VMEM((SIDES, chunks, planes, BLOCK_HEIGHT, HALF), F32),
            pltpu.VMEM((planes * BLOCK_HEIGHT, HALF), BF16),
            pltpu.VMEM((chunks, HALF, HALF), BF16),
            pltpu.VMEM((2, planes * BLOCK_HEIGHT, HALF), F32),
            pltpu.VMEM((2, 2, images * images * looks, HALF), BF16),
            pltpu.VMEM((SIDES, images * images * looks, HALF), F32),
            pltpu.VMEM((SIDES, 8, HALF // 2), F32),
            pltpu.VMEM((SIDES, 8, HALF // 2), F32),
            pltpu.VMEM((1, height), BF16),
            pltpu.SMEM((1, 1), I32),
            pltpu.SMEM((1, 2), I32),
            pltpu.SMEM((1, 2), I32),
            pltpu.SMEM((2, pairs), I32),
            pltpu.SemaphoreType.DMA((chunks,)),
            pltpu.SemaphoreType.DMA((5,)),
            pltpu.SemaphoreType.DMA((SIDES, chunks)),
            pltpu.SemaphoreType.DMA((SIDES, chunks)),
            pltpu.SemaphoreType.DMA((SIDES,)),
            pltpu.SemaphoreType.DMA((SIDES,)),
            pltpu.SemaphoreType.REGULAR,
        ],
        compiler_params=pltpu.CompilerParams(collective_id=0, has_side_effects=True),
    )(
        sweep_stack.reshape(planes, height, width),
        blend,
        start.reshape(1, 1),
        lines,
        columns,
        couples.T,
    )
    return pl.pallas_call(
        write,
        name="write",
        out_shape=(
            jax.ShapeDtypeStruct(ifg_shape, F32),
            jax.ShapeDtypeStruct(coh_shape, F32),
        ),
        in_specs=[vmem, vmem],
        out_specs=(hbm, hbm),
        scratch_shapes=[pltpu.SemaphoreType.DMA((2,))],
        compiler_params=pltpu.CompilerParams(vmem_limit_bytes=1024 * 1024),
    )(ifg, coh)


def solution(mesh):
    return jax.shard_map(
        functools.partial(per_device, mesh.shape["az"]),
        mesh=mesh,
        in_specs=(
            P(None, None, ("groups", "az"), None, None),
            P(("groups", "az"), None),
            P(("groups", "az")),
            P(("groups", "az"), None),
            P(("groups", "az"), None),
            P("groups", None),
        ),
        out_specs=(P(None, "groups", "az", None), P("groups", "az", None)),
        check_vma=False,
    )
```

```python
import functools

import jax
import jax.numpy as jnp
from jax import lax
from jax.experimental import pallas as pl
from jax.experimental.pallas import tpu as pltpu
from jax.sharding import PartitionSpec as P

BLOCK_HEIGHT = 40
LOOK_ROWS = 5
LOOK_COLS = 20
MARGIN = 15
HALF = 256
CHUNK = 2 * HALF
SUB = 16
SIDES = 2
F32, BF16, I32 = jnp.float32, jnp.bfloat16, jnp.int32
MESH = pl.DeviceIdType.MESH


def iota(shape, dimension):
    return lax.broadcasted_iota(I32, shape, dimension)


def dot(a, b):
    return jnp.dot(a, b, preferred_element_type=F32)


def swap(block):
    half = block.shape[0] // 2
    return jnp.concatenate([block[half:], block[:half]], axis=0)


def merge(
    ring,
    x_hbm,
    blend_hbm,
    start_hbm,
    lines_hbm,
    columns_hbm,
    couples_hbm,
    ifg_ref,
    coh_ref,
    x,
    stage,
    recv,
    own,
    spread,
    boxes,
    spilled,
    split,
    total,
    note,
    heard,
    blend,
    start,
    lines,
    columns,
    couples,
    x_sem,
    small_sem,
    send_sem,
    recv_sem,
    note_send,
    note_recv,
    hello,
):
    chunks, planes, height, _ = x.shape
    images = planes // 2
    pairs = couples.shape[1]
    looks = BLOCK_HEIGHT // LOOK_ROWS
    quads = looks // SIDES
    duos = [(i, j) for i in range(images) for j in range(i + 1, images)]
    me = lax.axis_index("az")
    above, below = lax.rem(me + ring - 1, ring), lax.rem(me + 1, ring)
    targets = (above, below)
    present = (me > 0, me < ring - 1)

    small = [
        pltpu.make_async_copy(source, target, small_sem.at[i])
        for i, (source, target) in enumerate(
            (
                (start_hbm, start),
                (columns_hbm, columns),
                (lines_hbm, lines),
                (blend_hbm, blend),
                (couples_hbm, couples),
            )
        )
    ]

    def load(c):
        return pltpu.make_async_copy(
            x_hbm.at[:, :, pl.ds(c * CHUNK, CHUNK)], x.at[c], x_sem.at[c]
        )

    for copy in small[:3]:
        copy.start()
    load(0).start()
    for copy in small[3:]:
        copy.start()
    for c in range(1, chunks):
        load(c).start()

    barrier = pltpu.get_barrier_semaphore()

    @pl.when(present[0])
    def _():
        pl.semaphore_signal(barrier, inc=1, device_id={"az": above}, device_id_type=MESH)

    for side in range(SIDES):

        @pl.when(jnp.logical_not(present[side]))
        def _():
            heard[side] = jnp.zeros(heard.shape[1:], F32)
            for c in range(chunks):
                recv[side, c] = jnp.zeros(recv.shape[2:], BF16)

    def outgoing(side, c):
        return pltpu.make_async_remote_copy(
            src_ref=stage.at[side, c],
            dst_ref=recv.at[1 - side, c],
            send_sem=send_sem.at[side, c],
            recv_sem=recv_sem.at[1 - side, c],
            device_id={"az": targets[side]},
            device_id_type=MESH,
        )

    def words(side):
        return pltpu.make_async_remote_copy(
            src_ref=note.at[side],
            dst_ref=heard.at[1 - side],
            send_sem=note_send.at[side],
            recv_sem=note_recv.at[1 - side],
            device_id={"az": targets[side]},
            device_id_type=MESH,
        )

    for copy in small[:2]:
        copy.wait()
    shift = start[0, 0] - me * BLOCK_HEIGHT
    bases = (-MARGIN, BLOCK_HEIGHT)

    place = iota((1, 2 * height), 1)
    second = place >= height
    line = jnp.where(second, place - height, place)
    row_of_line = line + shift

    lead = iota((SIDES * 2 * SUB, 1), 0)
    inner = lead % SUB
    leaves = jnp.where(lead < 2 * SUB, bases[0], bases[1]) + inner
    wanted = row_of_line == jnp.where(inner < MARGIN, leaves, -1000)
    half_matches = second == (lead % (2 * SUB) >= SUB)
    select = jnp.where(wanted & half_matches, 1.0, 0.0).astype(BF16)

    def masks(c):
        column = iota((1, CHUNK), 1) + c * CHUNK
        seen = (column >= columns[0, 0]) & (column < columns[0, 1])
        return jnp.where(seen, 1.0, 0.0).astype(BF16)

    def stacked(block):
        return jnp.concatenate([block[:, :HALF], block[:, HALF:]], axis=0)

    def prepare(c):
        load(c).wait()
        mask = masks(c)
        for p in range(planes):
            block = x[c, p] * mask
            x[c, p] = block
            out = dot(select, stacked(block)).astype(BF16)
            for side in range(SIDES):
                stage[side, c, pl.ds(2 * p * SUB, 2 * SUB), :] = out[
                    side * 2 * SUB : (side + 1) * 2 * SUB
                ]

    for copy in small[2:]:
        copy.wait()
    index = iota((1, height), 1)
    valid = (index >= lines[0, 0]) & (index < lines[0, 1])
    weight = jnp.where(valid, blend[...].astype(F32), 0.0)

    k = iota((height, 2 * HALF), 0)
    lane = iota((height, 2 * HALF), 1)
    inner = lane % SUB
    leaves = jnp.where(lane < HALF + HALF // 2, bases[0], bases[1]) + inner
    goes = (lane >= HALF) & (inner < MARGIN) & (k + shift == leaves)
    stays = (lane < HALF) & ((lane == k) | (lane == k + height))
    rows = jnp.broadcast_to(weight, (8, height)).astype(BF16)
    weights = dot(rows, jnp.where(goes | stays, 1.0, 0.0).astype(BF16))
    for side in range(SIDES):
        first = HALF + side * (HALF // 2)
        note[side] = weights[:, first : first + HALF // 2]
    twice = weights[:1, : 2 * height]

    @pl.when(present[1])
    def _():
        pl.semaphore_wait(barrier, 1)
        pl.semaphore_signal(hello, inc=1, device_id={"az": below}, device_id_type=MESH)
        words(1).start()

    for c in range(chunks):
        prepare(c)

        @pl.when(present[1])
        def _():
            outgoing(1, c).start()

    def send_up():
        pl.semaphore_wait(hello, 1)
        words(0).start()
        for c in range(chunks):
            outgoing(0, c).start()

    linked = me % 2 == 0

    @pl.when(present[0] & linked)
    def _():
        send_up()

    slot = iota((BLOCK_HEIGHT, 1), 0)
    quad = slot % quads
    second_slot = slot % looks >= quads
    row_in_side = LOOK_ROWS * quad + slot // looks
    keep_f32 = [
        jnp.where(
            (row_of_line == row_in_side + side * quads * LOOK_ROWS) & (second == second_slot),
            twice,
            0.0,
        )
        for side in range(SIDES)
    ]
    keep = jnp.concatenate(keep_f32, axis=0).astype(BF16)

    def held(c, carry):
        for p in range(planes):
            out = dot(keep, stacked(x[c, p]))
            for side in range(SIDES):
                own[side, c, p] = out[side * BLOCK_HEIGHT : (side + 1) * BLOCK_HEIGHT]
        return carry

    lax.fori_loop(0, chunks, held, 0)

    def box(c, carry):
        lane = iota((HALF, HALF), 1)
        far = lane >= HALF // 2
        sample = iota((HALF, HALF), 0) + c * CHUNK + jnp.where(far, HALF, 0)
        first = LOOK_COLS * jnp.where(far, lane - HALF // 2, lane)
        inside = (sample >= first) & (sample < first + LOOK_COLS)
        boxes[c] = jnp.where(inside, 1.0, 0.0).astype(BF16)
        return carry

    lax.fori_loop(0, chunks, box, 0)

    def settle(s, carry):
        side = lax.rem(me + s, 2)
        there = (side == 0) & present[0] | (side == 1) & present[1]

        @pl.when((s == 1) & present[0] & jnp.logical_not(linked))
        def _():
            send_up()

        @pl.when(there)
        def _():
            pltpu.make_async_remote_copy(
                src_ref=note.at[side],
                dst_ref=heard.at[side],
                send_sem=note_send.at[side],
                recv_sem=note_recv.at[side],
                device_id={"az": below},
                device_id_type=MESH,
            ).wait_recv()

        lane = iota((1, HALF), 1)
        tile, inner = lane // SUB, lane % SUB
        code = (tile % 2) * 64 + inner + side * LOOK_ROWS
        row_code = jnp.where(second_slot, 64, 0) + row_in_side
        matches = row_code == code
        incoming = jnp.concatenate([heard[side, :1, :]] * 2, axis=1)
        block = jnp.where(matches, incoming, 0.0)
        norm = jnp.sum(jnp.where(tile < 2, block, 0.0), axis=1, keepdims=True)
        stay = jnp.where(side == 0, keep_f32[0], keep_f32[1])
        norm = norm + jnp.sum(stay, axis=1, keepdims=True)
        scale = jnp.broadcast_to(1.0 / norm, (BLOCK_HEIGHT, HALF // 2))
        for p in range(planes):
            spread[pl.ds(p * BLOCK_HEIGHT, BLOCK_HEIGHT), :] = jnp.where(
                tile // 2 == p, block, 0.0
            ).astype(BF16)

        def arrive(c):
            @pl.when(there)
            def _():
                pltpu.make_async_remote_copy(
                    src_ref=stage.at[side, c],
                    dst_ref=recv.at[side, c],
                    send_sem=send_sem.at[side, c],
                    recv_sem=recv_sem.at[side, c],
                    device_id={"az": below},
                    device_id_type=MESH,
                ).wait_recv()

        def spill(c):
            spilled[c % 2] = dot(spread[...], recv[side, c])

        def products(c):
            for b in range(2):
                lanes = pl.ds(b * (HALF // 2), HALF // 2)
                sums = [None] * (images * images)

                def gather(at, value):
                    sums[at] = value if sums[at] is None else sums[at] + value

                for within in range(LOOK_ROWS):
                    own_rows = pl.ds(within * looks, looks)
                    factor = scale[within * looks : (within + 1) * looks]
                    merged = [
                        (
                            spilled[c % 2, pl.ds(p * BLOCK_HEIGHT + within * looks, looks), lanes]
                            + own[side, c, p, own_rows, lanes]
                        )
                        * factor
                        for p in range(planes)
                    ]
                    re, im = merged[:images], merged[images:]
                    for at, (i, j) in enumerate(duos):
                        gather(at, re[i] * re[j] + im[i] * im[j])
                        gather(len(duos) + at, im[i] * re[j] - re[i] * im[j])
                    for i in range(images):
                        gather(2 * len(duos) + i, re[i] * re[i] + im[i] * im[i])
                for at in range(0, images * images, 2):
                    value = jnp.concatenate(sums[at : at + 2], axis=0)
                    high = value.astype(BF16)
                    low = (value - high.astype(F32)).astype(BF16)
                    split[c % 2, 0, pl.ds(at * looks, 2 * looks), lanes] = high
                    split[c % 2, 1, pl.ds(at * looks, 2 * looks), lanes] = low

        def boxed(c):
            part = dot(split[c % 2, 0], boxes[c]) + dot(split[c % 2, 1], boxes[c])
            total[side] = part if c == 0 else total[side] + part

        for c in range(chunks + 2):
            if c < chunks:
                arrive(c)
                spill(c)
            if 1 <= c <= chunks:
                products(c - 1)
            if c >= 2:
                boxed(c - 2)
        return carry

    lax.fori_loop(0, SIDES, settle, 0)

    first_quads = iota((looks, HALF // 2), 0) < quads

    def looked(at):
        rows = pl.ds(at * looks, looks)
        left = [total[side, rows, pl.ds(0, HALF // 2)] for side in range(SIDES)]
        right = [total[side, rows, pl.ds(HALF // 2, HALF // 2)] for side in range(SIDES)]
        return jnp.where(first_quads, left[0] + swap(right[0]), swap(left[1]) + right[1])

    values = [looked(at) for at in range(images * images)]

    def splat(value):
        return jnp.full((looks, HALF // 2), value, I32)

    for p in range(pairs):
        i, j = splat(couples[0, p]), splat(couples[1, p])
        re = im = power_i = power_j = jnp.zeros(i.shape, F32)
        for at, (a, b) in enumerate(duos):
            forward = (i == a) & (j == b)
            backward = (i == b) & (j == a)
            re = jnp.where(forward | backward, values[at], re)
            im = jnp.where(forward, values[len(duos) + at], im)
            im = jnp.where(backward, -values[len(duos) + at], im)
        for a in range(images):
            power_i = jnp.where(i == a, values[2 * len(duos) + a], power_i)
            power_j = jnp.where(j == a, values[2 * len(duos) + a], power_j)
        ifg_ref[0, p] = re / (LOOK_ROWS * LOOK_COLS)
        ifg_ref[1, p] = im / (LOOK_ROWS * LOOK_COLS)
        coh_ref[p] = (re * re + im * im) / jnp.maximum(power_i * power_j, 1.0)

    for side in range(SIDES):

        @pl.when(present[side])
        def _():
            words(side).wait_send()
            for c in range(chunks):
                outgoing(side, c).wait_send()


def write(ifg_ref, coh_ref, ifg_hbm, coh_hbm, sems):
    copies = [
        pltpu.make_async_copy(ifg_ref, ifg_hbm, sems.at[0]),
        pltpu.make_async_copy(coh_ref, coh_hbm, sems.at[1]),
    ]
    for copy in copies:
        copy.start()
    for copy in copies:
        copy.wait()


def per_device(ring, sweep_stack, blend, start, lines, columns, couples):
    parts, images, _, height, width = sweep_stack.shape
    planes = parts * images
    pairs = couples.shape[0]
    chunks = width // CHUNK
    looks = BLOCK_HEIGHT // LOOK_ROWS
    outputs = width // LOOK_COLS
    hbm = pl.BlockSpec(memory_space=pltpu.HBM)
    vmem = pl.BlockSpec(memory_space=pltpu.VMEM)
    ifg_shape, coh_shape = (parts, pairs, looks, outputs), (pairs, looks, outputs)
    ifg, coh = pl.pallas_call(
        functools.partial(merge, ring),
        name="merge",
        out_shape=(pltpu.VMEM(ifg_shape, F32), pltpu.VMEM(coh_shape, F32)),
        in_specs=[hbm] * 6,
        out_specs=(vmem, vmem),
        scratch_shapes=[
            pltpu.VMEM((chunks, planes, height, CHUNK), BF16),
            pltpu.VMEM((SIDES, chunks, planes * 2 * SUB, HALF), BF16),
            pltpu.VMEM((SIDES, chunks, planes * 2 * SUB, HALF), BF16),
            pltpu.VMEM((SIDES, chunks, planes, BLOCK_HEIGHT, HALF), F32),
            pltpu.VMEM((planes * BLOCK_HEIGHT, HALF), BF16),
            pltpu.VMEM((chunks, HALF, HALF), BF16),
            pltpu.VMEM((2, planes * BLOCK_HEIGHT, HALF), F32),
            pltpu.VMEM((2, 2, images * images * looks, HALF), BF16),
            pltpu.VMEM((SIDES, images * images * looks, HALF), F32),
            pltpu.VMEM((SIDES, 8, HALF // 2), F32),
            pltpu.VMEM((SIDES, 8, HALF // 2), F32),
            pltpu.VMEM((1, height), BF16),
            pltpu.SMEM((1, 1), I32),
            pltpu.SMEM((1, 2), I32),
            pltpu.SMEM((1, 2), I32),
            pltpu.SMEM((2, pairs), I32),
            pltpu.SemaphoreType.DMA((chunks,)),
            pltpu.SemaphoreType.DMA((5,)),
            pltpu.SemaphoreType.DMA((SIDES, chunks)),
            pltpu.SemaphoreType.DMA((SIDES, chunks)),
            pltpu.SemaphoreType.DMA((SIDES,)),
            pltpu.SemaphoreType.DMA((SIDES,)),
            pltpu.SemaphoreType.REGULAR,
        ],
        compiler_params=pltpu.CompilerParams(collective_id=0, has_side_effects=True),
    )(
        sweep_stack.reshape(planes, height, width),
        blend,
        start.reshape(1, 1),
        lines,
        columns,
        couples.T,
    )
    return pl.pallas_call(
        write,
        name="write",
        out_shape=(
            jax.ShapeDtypeStruct(ifg_shape, F32),
            jax.ShapeDtypeStruct(coh_shape, F32),
        ),
        in_specs=[vmem, vmem],
        out_specs=(hbm, hbm),
        scratch_shapes=[pltpu.SemaphoreType.DMA((2,))],
        compiler_params=pltpu.CompilerParams(vmem_limit_bytes=1024 * 1024),
    )(ifg, coh)


def solution(mesh):
    return jax.shard_map(
        functools.partial(per_device, mesh.shape["az"]),
        mesh=mesh,
        in_specs=(
            P(None, None, ("groups", "az"), None, None),
            P(("groups", "az"), None),
            P(("groups", "az")),
            P(("groups", "az"), None),
            P(("groups", "az"), None),
            P("groups", None),
        ),
        out_specs=(P(None, "groups", "az", None), P("groups", "az", None)),
        check_vma=False,
    )
```

```python
import functools

import jax
import jax.numpy as jnp
from jax import lax
from jax.experimental import pallas as pl
from jax.experimental.pallas import tpu as pltpu
from jax.sharding import PartitionSpec as P

BLOCK_HEIGHT = 40
LOOK_ROWS = 5
LOOK_COLS = 20
MARGIN = 15
HALF = 256
CHUNK = 2 * HALF
SPILL_ROWS = 32
SIDES = 2
F32, BF16, I32 = jnp.float32, jnp.bfloat16, jnp.int32
MESH = pl.DeviceIdType.MESH


def iota(shape, dimension):
    return lax.broadcasted_iota(I32, shape, dimension)


def dot(a, b):
    return jnp.dot(a, b, preferred_element_type=F32)


def swap(block):
    half = block.shape[0] // 2
    return jnp.concatenate([block[half:], block[:half]], axis=0)


def merge(
    ring,
    x_hbm,
    blend_hbm,
    start_hbm,
    lines_hbm,
    columns_hbm,
    couples_hbm,
    ifg_ref,
    coh_ref,
    x,
    stage,
    recv,
    own,
    boxes,
    split,
    norms,
    total,
    note,
    heard,
    blend,
    start,
    lines,
    columns,
    couples,
    x_sem,
    small_sem,
    send_sem,
    recv_sem,
    note_send,
    note_recv,
    hello,
):
    chunks, planes, height, _ = x.shape
    images = planes // 2
    pairs = couples.shape[1]
    looks = BLOCK_HEIGHT // LOOK_ROWS
    quads = looks // SIDES
    duos = [(i, j) for i in range(images) for j in range(i + 1, images)]
    me = lax.axis_index("az")
    above, below = lax.rem(me + ring - 1, ring), lax.rem(me + 1, ring)
    targets = (above, below)
    present = (me > 0, me < ring - 1)

    small = [
        pltpu.make_async_copy(source, target, small_sem.at[i])
        for i, (source, target) in enumerate(
            (
                (start_hbm, start),
                (columns_hbm, columns),
                (lines_hbm, lines),
                (blend_hbm, blend),
                (couples_hbm, couples),
            )
        )
    ]

    def load(c):
        return pltpu.make_async_copy(
            x_hbm.at[:, :, pl.ds(c * CHUNK, CHUNK)], x.at[c], x_sem.at[c]
        )

    for copy in small:
        copy.start()
    load(0).start()
    barrier = pltpu.get_barrier_semaphore()

    @pl.when(present[0])
    def _():
        pl.semaphore_signal(barrier, inc=1, device_id={"az": above}, device_id_type=MESH)

    for c in range(1, chunks):
        load(c).start()

    for side in range(SIDES):

        @pl.when(jnp.logical_not(present[side]))
        def _():
            heard[side] = jnp.zeros(heard.shape[1:], F32)
            for c in range(chunks):
                recv[side, c] = jnp.zeros(recv.shape[2:], BF16)

    def outgoing(side, c):
        return pltpu.make_async_remote_copy(
            src_ref=stage.at[side, c],
            dst_ref=recv.at[1 - side, c],
            send_sem=send_sem.at[side, c],
            recv_sem=recv_sem.at[1 - side, c],
            device_id={"az": targets[side]},
            device_id_type=MESH,
        )

    def words(side):
        return pltpu.make_async_remote_copy(
            src_ref=note.at[side],
            dst_ref=heard.at[1 - side],
            send_sem=note_send.at[side],
            recv_sem=note_recv.at[1 - side],
            device_id={"az": targets[side]},
            device_id_type=MESH,
        )

    @pl.when(present[1])
    def _():
        pl.semaphore_wait(barrier, 1)
        pl.semaphore_signal(hello, inc=1, device_id={"az": below}, device_id_type=MESH)

    for copy in small[:4]:
        copy.wait()
    shift = start[0, 0] - me * BLOCK_HEIGHT
    bases = (-MARGIN, BLOCK_HEIGHT)

    place = iota((1, 2 * height), 1)
    second = place >= height
    line = jnp.where(second, place - height, place)
    row_of_line = line + shift

    def travels(rows):
        quad, register = rows % quads, rows // looks % quads
        row = jnp.where(quad < quads - 1, LOOK_ROWS * quad + register, LOOK_ROWS * (register + 1) - 1)
        return jnp.where((quad == quads - 1) & (register == quads - 1), -1000, row)

    lead = iota((SIDES * SPILL_ROWS, 1), 0)
    wanted = row_of_line == travels(lead) + jnp.where(lead < SPILL_ROWS, bases[0], bases[1])
    select = jnp.where(wanted & (second == (lead % looks >= quads)), 1.0, 0.0).astype(BF16)

    def masks(c):
        column = iota((1, CHUNK), 1) + c * CHUNK
        seen = (column >= columns[0, 0]) & (column < columns[0, 1])
        return jnp.where(seen, 1.0, 0.0).astype(BF16)

    def stacked(block):
        return jnp.concatenate([block[:, :HALF], block[:, HALF:]], axis=0)

    high_half = iota((SPILL_ROWS // 2, HALF), 0) % looks >= quads

    def prepare(c):
        load(c).wait()
        if c == 0:
            describe()
        mask = masks(c).astype(F32)
        mask = jnp.where(
            high_half,
            jnp.broadcast_to(mask[:, HALF:], high_half.shape),
            jnp.broadcast_to(mask[:, :HALF], high_half.shape),
        ).astype(BF16)
        mask = jnp.concatenate([mask] * (2 * SIDES), axis=0)
        for p in range(planes):
            out = dot(select, stacked(x[c, p])).astype(BF16) * mask
            for side in range(SIDES):
                stage[side, c, p] = out[side * SPILL_ROWS : (side + 1) * SPILL_ROWS]

    index = iota((1, height), 1)
    valid = (index >= lines[0, 0]) & (index < lines[0, 1])
    weight = jnp.where(valid, blend[...].astype(F32), 0.0)

    slot = iota((BLOCK_HEIGHT, 1), 0)
    quad, within_look = slot % quads, slot // looks
    second_slot = slot % looks >= quads

    def describe():
        for side in range(SIDES):
            goes = jnp.where(quad < quads - 1, LOOK_ROWS * quad + within_look + bases[side], -1000)
            sent = jnp.where(index + shift == goes, weight, 0.0)
            note[side] = jnp.broadcast_to(jnp.sum(sent, axis=1, keepdims=True), note.shape[1:])

    for c in range(chunks):
        prepare(c)

        @pl.when(present[1])
        def _():
            if c == 0:
                words(1).start()
            outgoing(1, c).start()

    def send_up():
        pl.semaphore_wait(hello, 1)
        words(0).start()
        for c in range(chunks):
            outgoing(0, c).start()

    linked = me % 2 == 0

    @pl.when(present[0] & linked)
    def _():
        send_up()

    k = iota((height, HALF), 0)
    lane = iota((height, HALF), 1)
    copies = jnp.where((lane == k) | (lane == k + height), 1.0, 0.0).astype(BF16)
    rows = jnp.broadcast_to(weight, (8, height)).astype(BF16)
    twice = dot(rows, copies)[:1, : 2 * height]

    keep = []
    for side in range(SIDES):
        look = quad if side == 0 else quads + (quad + 1) % quads
        stays = (row_of_line == LOOK_ROWS * look + within_look) & (second == second_slot)
        keep.append(jnp.where(stays, twice, 0.0))
        norms[side] = jnp.broadcast_to(
            jnp.sum(keep[side], axis=1, keepdims=True), norms.shape[1:]
        )
    keep = jnp.concatenate(keep, axis=0).astype(BF16)

    def held(c, carry):
        mask = masks(c)
        for p in range(planes):
            out = dot(keep, stacked(x[c, p] * mask))
            for side in range(SIDES):
                own[side, c, p] = out[side * BLOCK_HEIGHT : (side + 1) * BLOCK_HEIGHT]
        return carry

    lax.fori_loop(0, chunks, held, 0)

    def box(c, carry):
        lane = iota((HALF, HALF), 1)
        far = lane >= HALF // 2
        sample = iota((HALF, HALF), 0) + c * CHUNK + jnp.where(far, HALF, 0)
        first = LOOK_COLS * jnp.where(far, lane - HALF // 2, lane)
        inside = (sample >= first) & (sample < first + LOOK_COLS)
        boxes[c] = jnp.where(inside, 1.0, 0.0).astype(BF16)
        return carry

    lax.fori_loop(0, chunks, box, 0)

    def settle(s, carry):
        side = lax.rem(me + s, 2)
        there = (side == 0) & present[0] | (side == 1) & present[1]

        @pl.when((s == 1) & present[0] & jnp.logical_not(linked))
        def _():
            send_up()

        @pl.when(there)
        def _():
            pltpu.make_async_remote_copy(
                src_ref=note.at[side],
                dst_ref=heard.at[side],
                send_sem=note_send.at[side],
                recv_sem=note_recv.at[side],
                device_id={"az": below},
                device_id_type=MESH,
            ).wait_recv()

        scale = 1.0 / (norms[side] + heard[side])
        factor = heard[side] * scale

        def rescale(c, carry):
            for p in range(planes):
                for b in range(2):
                    lanes = pl.ds(b * (HALF // 2), HALF // 2)
                    own[side, c, p, :, lanes] = own[side, c, p, :, lanes] * scale
            return carry

        lax.fori_loop(0, chunks, rescale, 0)
        third = iota((looks, HALF // 2), 0) % quads

        def arrive(c):
            @pl.when(there)
            def _():
                pltpu.make_async_remote_copy(
                    src_ref=stage.at[side, c],
                    dst_ref=recv.at[side, c],
                    send_sem=send_sem.at[side, c],
                    recv_sem=recv_sem.at[side, c],
                    device_id={"az": below},
                    device_id_type=MESH,
                ).wait_recv()

        def products(c):
            for b in range(2):
                lanes = pl.ds(b * (HALF // 2), HALF // 2)
                sums = [None] * (images * images)

                def gather(at, value):
                    sums[at] = value if sums[at] is None else sums[at] + value

                spills = []
                for p in range(planes):
                    block = recv[side, c, p, :, lanes].astype(F32)
                    parts = [block[v * looks : (v + 1) * looks] for v in range(quads)]
                    turned = [
                        pltpu.roll(parts[v], looks - (quads - 1) + v, 0) for v in range(quads - 1)
                    ]
                    last = turned[quads - 2]
                    for v in range(quads - 2):
                        last = jnp.where(third == v, turned[v], last)
                    spills.append(parts + [last])

                for within in range(LOOK_ROWS):
                    rows = pl.ds(within * looks, looks)
                    weights = factor[within * looks : (within + 1) * looks]
                    merged = [
                        own[side, c, p, rows, lanes] + spills[p][within] * weights
                        for p in range(planes)
                    ]
                    re, im = merged[:images], merged[images:]
                    for at, (i, j) in enumerate(duos):
                        gather(at, re[i] * re[j] + im[i] * im[j])
                        gather(len(duos) + at, im[i] * re[j] - re[i] * im[j])
                    for i in range(images):
                        gather(2 * len(duos) + i, re[i] * re[i] + im[i] * im[i])
                for at in range(0, images * images, 2):
                    value = jnp.concatenate(sums[at : at + 2], axis=0)
                    high = value.astype(BF16)
                    low = (value - high.astype(F32)).astype(BF16)
                    split[c % 2, 0, pl.ds(at * looks, 2 * looks), lanes] = high
                    split[c % 2, 1, pl.ds(at * looks, 2 * looks), lanes] = low

        def boxed(c):
            part = dot(split[c % 2, 0], boxes[c]) + dot(split[c % 2, 1], boxes[c])
            total[side] = part if c == 0 else total[side] + part

        for c in range(chunks + 1):
            if c < chunks:
                arrive(c)
                products(c)
            if c >= 1:
                boxed(c - 1)
        return carry

    lax.fori_loop(0, SIDES, settle, 0)

    small[4].wait()
    sublane = iota((looks, HALF // 2), 0)

    def looked(at):
        rows = pl.ds(at * looks, looks)
        left = [total[side, rows, pl.ds(0, HALF // 2)] for side in range(SIDES)]
        right = [total[side, rows, pl.ds(HALF // 2, HALF // 2)] for side in range(SIDES)]
        top, bottom = [left[side] + swap(right[side]) for side in range(SIDES)]
        bottom = jnp.where(
            sublane == quads, pltpu.roll(bottom, 1, 0), pltpu.roll(bottom, quads + 1, 0)
        )
        return jnp.where(sublane < quads, top, bottom)

    values = [looked(at) for at in range(images * images)]

    def splat(value):
        return jnp.full((looks, HALF // 2), value, I32)

    for p in range(pairs):
        i, j = splat(couples[0, p]), splat(couples[1, p])
        re = im = power_i = power_j = jnp.zeros(i.shape, F32)
        for at, (a, b) in enumerate(duos):
            forward = (i == a) & (j == b)
            backward = (i == b) & (j == a)
            re = jnp.where(forward | backward, values[at], re)
            im = jnp.where(forward, values[len(duos) + at], im)
            im = jnp.where(backward, -values[len(duos) + at], im)
        for a in range(images):
            power_i = jnp.where(i == a, values[2 * len(duos) + a], power_i)
            power_j = jnp.where(j == a, values[2 * len(duos) + a], power_j)
        ifg_ref[0, p] = re / (LOOK_ROWS * LOOK_COLS)
        ifg_ref[1, p] = im / (LOOK_ROWS * LOOK_COLS)
        coh_ref[p] = (re * re + im * im) / jnp.maximum(power_i * power_j, 1.0)

    for side in range(SIDES):

        @pl.when(present[side])
        def _():
            words(side).wait_send()
            for c in range(chunks):
                outgoing(side, c).wait_send()


def write(ifg_ref, coh_ref, ifg_hbm, coh_hbm, sems):
    copies = [
        pltpu.make_async_copy(ifg_ref, ifg_hbm, sems.at[0]),
        pltpu.make_async_copy(coh_ref, coh_hbm, sems.at[1]),
    ]
    for copy in copies:
        copy.start()
    for copy in copies:
        copy.wait()


def per_device(ring, sweep_stack, blend, start, lines, columns, couples):
    parts, images, _, height, width = sweep_stack.shape
    planes = parts * images
    pairs = couples.shape[0]
    chunks = width // CHUNK
    looks = BLOCK_HEIGHT // LOOK_ROWS
    outputs = width // LOOK_COLS
    hbm = pl.BlockSpec(memory_space=pltpu.HBM)
    vmem = pl.BlockSpec(memory_space=pltpu.VMEM)
    ifg_shape, coh_shape = (parts, pairs, looks, outputs), (pairs, looks, outputs)
    ifg, coh = pl.pallas_call(
        functools.partial(merge, ring),
        name="merge",
        out_shape=(pltpu.VMEM(ifg_shape, F32), pltpu.VMEM(coh_shape, F32)),
        in_specs=[hbm] * 6,
        out_specs=(vmem, vmem),
        scratch_shapes=[
            pltpu.VMEM((chunks, planes, height, CHUNK), BF16),
            pltpu.VMEM((SIDES, chunks, planes, SPILL_ROWS, HALF), BF16),
            pltpu.VMEM((SIDES, chunks, planes, SPILL_ROWS, HALF), BF16),
            pltpu.VMEM((SIDES, chunks, planes, BLOCK_HEIGHT, HALF), F32),
            pltpu.VMEM((chunks, HALF, HALF), BF16),
            pltpu.VMEM((2, 2, images * images * looks, HALF), BF16),
            pltpu.VMEM((SIDES, BLOCK_HEIGHT, HALF // 2), F32),
            pltpu.VMEM((SIDES, images * images * looks, HALF), F32),
            pltpu.VMEM((SIDES, BLOCK_HEIGHT, HALF // 2), F32),
            pltpu.VMEM((SIDES, BLOCK_HEIGHT, HALF // 2), F32),
            pltpu.VMEM((1, height), BF16),
            pltpu.SMEM((1, 1), I32),
            pltpu.SMEM((1, 2), I32),
            pltpu.SMEM((1, 2), I32),
            pltpu.SMEM((2, pairs), I32),
            pltpu.SemaphoreType.DMA((chunks,)),
            pltpu.SemaphoreType.DMA((5,)),
            pltpu.SemaphoreType.DMA((SIDES, chunks)),
            pltpu.SemaphoreType.DMA((SIDES, chunks)),
            pltpu.SemaphoreType.DMA((SIDES,)),
            pltpu.SemaphoreType.DMA((SIDES,)),
            pltpu.SemaphoreType.REGULAR,
        ],
        compiler_params=pltpu.CompilerParams(collective_id=0, has_side_effects=True),
    )(
        sweep_stack.reshape(planes, height, width),
        blend,
        start.reshape(1, 1),
        lines,
        columns,
        couples.T,
    )
    return pl.pallas_call(
        write,
        name="write",
        out_shape=(
            jax.ShapeDtypeStruct(ifg_shape, F32),
            jax.ShapeDtypeStruct(coh_shape, F32),
        ),
        in_specs=[vmem, vmem],
        out_specs=(hbm, hbm),
        scratch_shapes=[pltpu.SemaphoreType.DMA((2,))],
        compiler_params=pltpu.CompilerParams(vmem_limit_bytes=1024 * 1024),
    )(ifg, coh)


def solution(mesh):
    return jax.shard_map(
        functools.partial(per_device, mesh.shape["az"]),
        mesh=mesh,
        in_specs=(
            P(None, None, ("groups", "az"), None, None),
            P(("groups", "az"), None),
            P(("groups", "az")),
            P(("groups", "az"), None),
            P(("groups", "az"), None),
            P("groups", None),
        ),
        out_specs=(P(None, "groups", "az", None), P("groups", "az", None)),
        check_vma=False,
    )
```

```python
import functools

import jax
import jax.numpy as jnp
from jax import lax
from jax.experimental import pallas as pl
from jax.experimental.pallas import tpu as pltpu
from jax.sharding import PartitionSpec as P

BLOCK_HEIGHT = 40
LOOK_ROWS = 5
LOOK_COLS = 20
MARGIN = 15
HALF = 256
CHUNK = 2 * HALF
SPILL_ROWS = 32
SIDES = 2
F32, BF16, I32 = jnp.float32, jnp.bfloat16, jnp.int32
MESH = pl.DeviceIdType.MESH


def iota(shape, dimension):
    return lax.broadcasted_iota(I32, shape, dimension)


def dot(a, b):
    return jnp.dot(a, b, preferred_element_type=F32)


def swap(block):
    half = block.shape[0] // 2
    return jnp.concatenate([block[half:], block[:half]], axis=0)


def merge(
    ring,
    x_hbm,
    blend_hbm,
    start_hbm,
    lines_hbm,
    columns_hbm,
    couples_hbm,
    ifg_ref,
    coh_ref,
    x,
    stage,
    recv,
    own,
    boxes,
    split,
    norms,
    total,
    note,
    heard,
    blend,
    start,
    lines,
    columns,
    couples,
    x_sem,
    small_sem,
    send_sem,
    recv_sem,
    note_send,
    note_recv,
    hello,
):
    chunks, planes, height, _ = x.shape
    images = planes // 2
    pairs = couples.shape[1]
    looks = BLOCK_HEIGHT // LOOK_ROWS
    quads = looks // SIDES
    duos = [(i, j) for i in range(images) for j in range(i + 1, images)]
    me = lax.axis_index("az")
    above, below = lax.rem(me + ring - 1, ring), lax.rem(me + 1, ring)
    targets = (above, below)
    present = (me > 0, me < ring - 1)

    small = [
        pltpu.make_async_copy(source, target, small_sem.at[i])
        for i, (source, target) in enumerate(
            (
                (start_hbm, start),
                (columns_hbm, columns),
                (lines_hbm, lines),
                (blend_hbm, blend),
                (couples_hbm, couples),
            )
        )
    ]

    def load(c):
        return pltpu.make_async_copy(
            x_hbm.at[:, :, pl.ds(c * CHUNK, CHUNK)], x.at[c], x_sem.at[c]
        )

    for copy in small:
        copy.start()
    load(0).start()
    barrier = pltpu.get_barrier_semaphore()

    @pl.when(present[0])
    def _():
        pl.semaphore_signal(barrier, inc=1, device_id={"az": above}, device_id_type=MESH)

    for c in range(1, chunks):
        load(c).start()

    for side in range(SIDES):

        @pl.when(jnp.logical_not(present[side]))
        def _():
            heard[side] = jnp.zeros(heard.shape[1:], F32)
            for c in range(chunks):
                recv[side, c] = jnp.zeros(recv.shape[2:], BF16)

    def outgoing(side, c):
        return pltpu.make_async_remote_copy(
            src_ref=stage.at[side, c],
            dst_ref=recv.at[1 - side, c],
            send_sem=send_sem.at[side, c],
            recv_sem=recv_sem.at[1 - side, c],
            device_id={"az": targets[side]},
            device_id_type=MESH,
        )

    def words(side):
        return pltpu.make_async_remote_copy(
            src_ref=note.at[side],
            dst_ref=heard.at[1 - side],
            send_sem=note_send.at[side],
            recv_sem=note_recv.at[1 - side],
            device_id={"az": targets[side]},
            device_id_type=MESH,
        )

    @pl.when(present[1])
    def _():
        pl.semaphore_wait(barrier, 1)
        pl.semaphore_signal(hello, inc=1, device_id={"az": below}, device_id_type=MESH)

    for copy in small[:4]:
        copy.wait()
    shift = start[0, 0] - me * BLOCK_HEIGHT
    bases = (-MARGIN, BLOCK_HEIGHT)

    place = iota((1, 2 * height), 1)
    second = place >= height
    line = jnp.where(second, place - height, place)
    row_of_line = line + shift

    def travels(rows):
        quad, register = rows % quads, rows // looks % quads
        row = jnp.where(quad < quads - 1, LOOK_ROWS * quad + register, LOOK_ROWS * (register + 1) - 1)
        return jnp.where((quad == quads - 1) & (register == quads - 1), -1000, row)

    lead = iota((SIDES * SPILL_ROWS, 1), 0)
    wanted = row_of_line == travels(lead) + jnp.where(lead < SPILL_ROWS, bases[0], bases[1])
    select = jnp.where(wanted & (second == (lead % looks >= quads)), 1.0, 0.0).astype(BF16)

    def masks(c):
        column = iota((1, CHUNK), 1) + c * CHUNK
        seen = (column >= columns[0, 0]) & (column < columns[0, 1])
        return jnp.where(seen, 1.0, 0.0).astype(BF16)

    def stacked(block):
        return jnp.concatenate([block[:, :HALF], block[:, HALF:]], axis=0)

    high_half = iota((SPILL_ROWS // 2, HALF), 0) % looks >= quads

    def prepare(c):
        load(c).wait()
        if c == 0:
            describe()
        mask = masks(c).astype(F32)
        mask = jnp.where(
            high_half,
            jnp.broadcast_to(mask[:, HALF:], high_half.shape),
            jnp.broadcast_to(mask[:, :HALF], high_half.shape),
        ).astype(BF16)
        mask = jnp.concatenate([mask] * (2 * SIDES), axis=0)
        for p in range(planes):
            out = dot(select, stacked(x[c, p])).astype(BF16) * mask
            for side in range(SIDES):
                stage[side, c, p] = out[side * SPILL_ROWS : (side + 1) * SPILL_ROWS]

    index = iota((1, height), 1)
    valid = (index >= lines[0, 0]) & (index < lines[0, 1])
    weight = jnp.where(valid, blend[...].astype(F32), 0.0)

    slot = iota((BLOCK_HEIGHT, 1), 0)
    quad, within_look = slot % quads, slot // looks
    second_slot = slot % looks >= quads

    def describe():
        for side in range(SIDES):
            goes = jnp.where(quad < quads - 1, LOOK_ROWS * quad + within_look + bases[side], -1000)
            sent = jnp.where(index + shift == goes, weight, 0.0)
            note[side] = jnp.broadcast_to(jnp.sum(sent, axis=1, keepdims=True), note.shape[1:])

    linked = me % 2 == 0

    def greet():
        pl.semaphore_wait(hello, 1)
        words(0).start()

    for c in range(chunks):
        prepare(c)

        @pl.when(present[1])
        def _():
            if c == 0:
                words(1).start()
            outgoing(1, c).start()

        if c == 1:

            @pl.when(present[0] & linked)
            def _():
                greet()
                for earlier in range(c + 1):
                    outgoing(0, earlier).start()

        elif c > 1:

            @pl.when(present[0] & linked)
            def _():
                outgoing(0, c).start()

    k = iota((height, HALF), 0)
    lane = iota((height, HALF), 1)
    copies = jnp.where((lane == k) | (lane == k + height), 1.0, 0.0).astype(BF16)
    rows = jnp.broadcast_to(weight, (8, height)).astype(BF16)
    twice = dot(rows, copies)[:1, : 2 * height]

    keep = []
    for side in range(SIDES):
        look = quad if side == 0 else quads + (quad + 1) % quads
        stays = (row_of_line == LOOK_ROWS * look + within_look) & (second == second_slot)
        keep.append(jnp.where(stays, twice, 0.0))
        norms[side] = jnp.broadcast_to(
            jnp.sum(keep[side], axis=1, keepdims=True), norms.shape[1:]
        )
    keep = jnp.concatenate(keep, axis=0).astype(BF16)

    def held(c, carry):
        mask = masks(c)
        for p in range(planes):
            out = dot(keep, stacked(x[c, p] * mask))
            for side in range(SIDES):
                own[side, c, p] = out[side * BLOCK_HEIGHT : (side + 1) * BLOCK_HEIGHT]
        return carry

    lax.fori_loop(0, chunks, held, 0)

    def box(c, carry):
        lane = iota((HALF, HALF), 1)
        far = lane >= HALF // 2
        sample = iota((HALF, HALF), 0) + c * CHUNK + jnp.where(far, HALF, 0)
        first = LOOK_COLS * jnp.where(far, lane - HALF // 2, lane)
        inside = (sample >= first) & (sample < first + LOOK_COLS)
        boxes[c] = jnp.where(inside, 1.0, 0.0).astype(BF16)
        return carry

    lax.fori_loop(0, chunks, box, 0)

    @pl.when(present[0] & jnp.logical_not(linked))
    def _():
        greet()
        for c in range(chunks):
            outgoing(0, c).start()

    def settle(s, carry):
        side = lax.rem(me + s, 2)
        there = (side == 0) & present[0] | (side == 1) & present[1]

        @pl.when(there)
        def _():
            pltpu.make_async_remote_copy(
                src_ref=note.at[side],
                dst_ref=heard.at[side],
                send_sem=note_send.at[side],
                recv_sem=note_recv.at[side],
                device_id={"az": below},
                device_id_type=MESH,
            ).wait_recv()

        scale = 1.0 / (norms[side] + heard[side])
        factor = heard[side] * scale

        def rescale(c, carry):
            for p in range(planes):
                for b in range(2):
                    lanes = pl.ds(b * (HALF // 2), HALF // 2)
                    own[side, c, p, :, lanes] = own[side, c, p, :, lanes] * scale
            return carry

        lax.fori_loop(0, chunks, rescale, 0)
        third = iota((looks, HALF // 2), 0) % quads

        def arrive(c):
            @pl.when(there)
            def _():
                pltpu.make_async_remote_copy(
                    src_ref=stage.at[side, c],
                    dst_ref=recv.at[side, c],
                    send_sem=send_sem.at[side, c],
                    recv_sem=recv_sem.at[side, c],
                    device_id={"az": below},
                    device_id_type=MESH,
                ).wait_recv()

        def products(c):
            for b in range(2):
                lanes = pl.ds(b * (HALF // 2), HALF // 2)
                sums = [None] * (images * images)

                def gather(at, value):
                    sums[at] = value if sums[at] is None else sums[at] + value

                spills = []
                for p in range(planes):
                    block = recv[side, c, p, :, lanes].astype(F32)
                    parts = [block[v * looks : (v + 1) * looks] for v in range(quads)]
                    turned = [
                        pltpu.roll(parts[v], looks - (quads - 1) + v, 0) for v in range(quads - 1)
                    ]
                    last = turned[quads - 2]
                    for v in range(quads - 2):
                        last = jnp.where(third == v, turned[v], last)
                    spills.append(parts + [last])

                for within in range(LOOK_ROWS):
                    rows = pl.ds(within * looks, looks)
                    weights = factor[within * looks : (within + 1) * looks]
                    merged = [
                        own[side, c, p, rows, lanes] + spills[p][within] * weights
                        for p in range(planes)
                    ]
                    re, im = merged[:images], merged[images:]
                    for at, (i, j) in enumerate(duos):
                        gather(at, re[i] * re[j] + im[i] * im[j])
                        gather(len(duos) + at, im[i] * re[j] - re[i] * im[j])
                    for i in range(images):
                        gather(2 * len(duos) + i, re[i] * re[i] + im[i] * im[i])
                for at in range(0, images * images, 2):
                    value = jnp.concatenate(sums[at : at + 2], axis=0)
                    high = value.astype(BF16)
                    low = (value - high.astype(F32)).astype(BF16)
                    split[c % 2, 0, pl.ds(at * looks, 2 * looks), lanes] = high
                    split[c % 2, 1, pl.ds(at * looks, 2 * looks), lanes] = low

        def boxed(c):
            part = dot(split[c % 2, 0], boxes[c]) + dot(split[c % 2, 1], boxes[c])
            total[side] = part if c == 0 else total[side] + part

        for c in range(chunks + 1):
            if c < chunks:
                arrive(c)
                products(c)
            if c >= 1:
                boxed(c - 1)
        return carry

    lax.fori_loop(0, SIDES, settle, 0)

    small[4].wait()
    sublane = iota((looks, HALF // 2), 0)

    def looked(at):
        rows = pl.ds(at * looks, looks)
        left = [total[side, rows, pl.ds(0, HALF // 2)] for side in range(SIDES)]
        right = [total[side, rows, pl.ds(HALF // 2, HALF // 2)] for side in range(SIDES)]
        top, bottom = [left[side] + swap(right[side]) for side in range(SIDES)]
        bottom = jnp.where(
            sublane == quads, pltpu.roll(bottom, 1, 0), pltpu.roll(bottom, quads + 1, 0)
        )
        return jnp.where(sublane < quads, top, bottom)

    values = [looked(at) for at in range(images * images)]

    def splat(value):
        return jnp.full((looks, HALF // 2), value, I32)

    for p in range(pairs):
        i, j = splat(couples[0, p]), splat(couples[1, p])
        re = im = power_i = power_j = jnp.zeros(i.shape, F32)
        for at, (a, b) in enumerate(duos):
            forward = (i == a) & (j == b)
            backward = (i == b) & (j == a)
            re = jnp.where(forward | backward, values[at], re)
            im = jnp.where(forward, values[len(duos) + at], im)
            im = jnp.where(backward, -values[len(duos) + at], im)
        for a in range(images):
            power_i = jnp.where(i == a, values[2 * len(duos) + a], power_i)
            power_j = jnp.where(j == a, values[2 * len(duos) + a], power_j)
        ifg_ref[0, p] = re / (LOOK_ROWS * LOOK_COLS)
        ifg_ref[1, p] = im / (LOOK_ROWS * LOOK_COLS)
        coh_ref[p] = (re * re + im * im) / jnp.maximum(power_i * power_j, 1.0)

    for side in range(SIDES):

        @pl.when(present[side])
        def _():
            words(side).wait_send()
            for c in range(chunks):
                outgoing(side, c).wait_send()


def write(ifg_ref, coh_ref, ifg_hbm, coh_hbm, sems):
    copies = [
        pltpu.make_async_copy(ifg_ref, ifg_hbm, sems.at[0]),
        pltpu.make_async_copy(coh_ref, coh_hbm, sems.at[1]),
    ]
    for copy in copies:
        copy.start()
    for copy in copies:
        copy.wait()


def per_device(ring, sweep_stack, blend, start, lines, columns, couples):
    parts, images, _, height, width = sweep_stack.shape
    planes = parts * images
    pairs = couples.shape[0]
    chunks = width // CHUNK
    looks = BLOCK_HEIGHT // LOOK_ROWS
    outputs = width // LOOK_COLS
    hbm = pl.BlockSpec(memory_space=pltpu.HBM)
    vmem = pl.BlockSpec(memory_space=pltpu.VMEM)
    ifg_shape, coh_shape = (parts, pairs, looks, outputs), (pairs, looks, outputs)
    ifg, coh = pl.pallas_call(
        functools.partial(merge, ring),
        name="merge",
        out_shape=(pltpu.VMEM(ifg_shape, F32), pltpu.VMEM(coh_shape, F32)),
        in_specs=[hbm] * 6,
        out_specs=(vmem, vmem),
        scratch_shapes=[
            pltpu.VMEM((chunks, planes, height, CHUNK), BF16),
            pltpu.VMEM((SIDES, chunks, planes, SPILL_ROWS, HALF), BF16),
            pltpu.VMEM((SIDES, chunks, planes, SPILL_ROWS, HALF), BF16),
            pltpu.VMEM((SIDES, chunks, planes, BLOCK_HEIGHT, HALF), F32),
            pltpu.VMEM((chunks, HALF, HALF), BF16),
            pltpu.VMEM((2, 2, images * images * looks, HALF), BF16),
            pltpu.VMEM((SIDES, BLOCK_HEIGHT, HALF // 2), F32),
            pltpu.VMEM((SIDES, images * images * looks, HALF), F32),
            pltpu.VMEM((SIDES, BLOCK_HEIGHT, HALF // 2), F32),
            pltpu.VMEM((SIDES, BLOCK_HEIGHT, HALF // 2), F32),
            pltpu.VMEM((1, height), BF16),
            pltpu.SMEM((1, 1), I32),
            pltpu.SMEM((1, 2), I32),
            pltpu.SMEM((1, 2), I32),
            pltpu.SMEM((2, pairs), I32),
            pltpu.SemaphoreType.DMA((chunks,)),
            pltpu.SemaphoreType.DMA((5,)),
            pltpu.SemaphoreType.DMA((SIDES, chunks)),
            pltpu.SemaphoreType.DMA((SIDES, chunks)),
            pltpu.SemaphoreType.DMA((SIDES,)),
            pltpu.SemaphoreType.DMA((SIDES,)),
            pltpu.SemaphoreType.REGULAR,
        ],
        compiler_params=pltpu.CompilerParams(collective_id=0, has_side_effects=True),
    )(
        sweep_stack.reshape(planes, height, width),
        blend,
        start.reshape(1, 1),
        lines,
        columns,
        couples.T,
    )
    return pl.pallas_call(
        write,
        name="write",
        out_shape=(
            jax.ShapeDtypeStruct(ifg_shape, F32),
            jax.ShapeDtypeStruct(coh_shape, F32),
        ),
        in_specs=[vmem, vmem],
        out_specs=(hbm, hbm),
        scratch_shapes=[pltpu.SemaphoreType.DMA((2,))],
        compiler_params=pltpu.CompilerParams(vmem_limit_bytes=1024 * 1024),
    )(ifg, coh)


def solution(mesh):
    return jax.shard_map(
        functools.partial(per_device, mesh.shape["az"]),
        mesh=mesh,
        in_specs=(
            P(None, None, ("groups", "az"), None, None),
            P(("groups", "az"), None),
            P(("groups", "az")),
            P(("groups", "az"), None),
            P(("groups", "az"), None),
            P("groups", None),
        ),
        out_specs=(P(None, "groups", "az", None), P("groups", "az", None)),
        check_vma=False,
    )
```
